512 devices in a mesh: ens: 2 (over y), gx: 32 (over z), col: 4 (over x), gz: 2 (over core).
Axes of the slice: x: 4, y: 2, z: 32, core: 2. Of those that a mesh axis runs over, the one named last changes fastest.
The devices are a block of a 4x8x32 slice.
Arguments:
- checkpoints: bfloat16 [8, 3, 32, 64, 512], P(('ens', 'col'), None, 'gz', 'gx'), parts along dimension 0, may hold values from -3 to 3
- obs_values: float32 [8, 32, 64, 512], P('ens', 'gz', 'gx', 'col'), parts along dimension 0, may hold values from -3 to 3
- obs_mask: int32 [8, 32, 64, 512], P('ens', 'gz', 'gx', 'col'), parts along dimension 0, may hold values 0 or 1
- drag: float32 [64], P(('ens', 'gz')), parts along dimension 0, may hold values from 0.05 to 0.5
Outputs:
- grad_init: float32 [6, 32, 64, 512], P('ens', 'gz', 'gx', 'col'), parts along dimension 0
- cost_levels: float32 [64], P(('ens', 'gz')), parts along dimension 0
- drag_grad: float32 [64], P(('ens', 'gz')), parts along dimension 0
The draws below stay inside these ranges and needn't reach their ends.
There are 2 independent parts, one for each index of `ens`. The reference program is written for one: setup_inputs(seed, part) draws one part's arguments, and reference() takes and returns one part's arrays. A program takes and returns all parts, laid end to end along the dimension named above; each array names one. Nothing has to cross between parts.
All inputs are finite; a program needn't handle non-finite values. No bound on the sum of `obs_mask` on one device may be relied on, other than what follows from the above.
Results may differ from the reference program's by a relative error of at most 0.0003.
Values may be sent and summed in bfloat16 or wider, within the bound.
No kernel may reach another device: no remote copies, remote signals or barrier semaphores. Data moves between devices by JAX's collectives and lax.ppermute only.
A program may use at most 64 MiB of HBM per device.

```python
import math
import jax
import jax.numpy as jnp
from jax import lax

NLEV = 32
NSEG = 4
SEG = 2
NX = 64
NY = 512


def set_ends(array, own_key, smallest, largest):
    spot = [jax.random.randint(jax.random.fold_in(own_key, axis), (), 0, length) for axis, length in enumerate(array.shape)]
    longest = array.shape.index(max(array.shape))
    next_to = spot[:longest] + [(spot[longest] + 1) % array.shape[longest]] + spot[longest + 1:]
    return array.at[tuple(spot)].set(smallest).at[tuple(next_to)].set(largest)


def level_of(rng, dims, pieces, least, high):
    def one(position, blocks):
        steps = jax.random.uniform(jax.random.fold_in(jax.random.fold_in(rng, 6), position), (blocks,), jnp.float32, least / len(pieces), high / len(pieces))
        return jnp.repeat(jnp.exp(steps), dims[position] // blocks).reshape((-1,) + (1,) * (len(dims) - position - 1))

    loudness = one(*pieces[0])
    for cut in pieces[1:]:
        loudness = loudness * one(*cut)
    return loudness


def bell_draw(rng, shape, spread, limit, split=(), dtype=jnp.bfloat16):
    result = jax.random.normal(rng, shape, jnp.float32) * spread
    if len(split) > 0:
        result = level_of(rng, shape, split, -0.22, 0.18) * result
    return jnp.clip(result, min=-limit, max=limit).astype(dtype)


def setup_inputs(seed: int = 0, part: int = 0) -> dict:
    seeds = jax.random.split(jax.random.key(seed), 5)
    part_splits = jax.random.split(jax.random.fold_in(seeds[4], part), 5)
    checkpoints = bell_draw(part_splits[0], (NSEG, 3, NLEV, NX, NY), 0.5, 3.0, ((0, 4), (2, 2), (3, 32)))
    obs_values = bell_draw(part_splits[1], (NSEG, NLEV, NX, NY), 0.5, 3.0, ((1, 2), (2, 32), (3, 4)), jnp.float32)
    obs_mask = set_ends((jax.random.randint(part_splits[2], (NSEG, NLEV, NX, NY), 0, 3) < 1).astype(jnp.int32), jax.random.fold_in(part_splits[2], 1), 0, 1)
    drag = jnp.clip(jnp.exp(math.log(0.5) - 2.3025851 * jax.random.uniform(part_splits[3], (NLEV,), jnp.float32) ** level_of(part_splits[3], (NLEV,), ((0, 2),), -0.2, 0.2)), 0.05, 0.5)
    return {"checkpoints": checkpoints, "obs_values": obs_values, "obs_mask": obs_mask, "drag": drag}


time_step = 0.1
viscosity = 0.05
vertical_mix = 0.2

def along_cols(a):
    return 0.5 * (a[:, 1:-1, 2:] - a[:, 1:-1, :-2])

def along_rows(a):
    return 0.5 * (a[:, 2:, 1:-1] - a[:, :-2, 1:-1])

def laplace(a):
    return a[:, 2:, 1:-1] + a[:, :-2, 1:-1] + a[:, 1:-1, 2:] + a[:, 1:-1, :-2] - 4.0 * a[:, 1:-1, 1:-1]

def advance(padded, drag, coriolis):
    levels = padded[:, 1:-1]
    thick, zonal, merid = (levels[0], levels[1], levels[2])
    centre = padded[:, 1:-1, 1:-1, 1:-1]
    h_c, u_c, v_c = (centre[0], centre[1], centre[2])
    rot = coriolis[None, :, None]
    rate = drag[:, None, None]
    vert = padded[:, 2:, 1:-1, 1:-1] + padded[:, :-2, 1:-1, 1:-1] - 2.0 * centre
    u_new = u_c + time_step * (-along_cols(thick) - u_c * along_cols(zonal) - v_c * along_rows(zonal) + rot * v_c - rate * u_c) + viscosity * laplace(zonal)
    v_new = v_c + time_step * (-along_rows(thick) - u_c * along_cols(merid) - v_c * along_rows(merid) - rot * u_c - rate * v_c) + viscosity * laplace(merid)
    h_new = h_c - time_step * (along_cols(zonal) + along_rows(merid) + along_cols(thick * zonal) + along_rows(thick * merid)) + viscosity * laplace(thick)
    return jnp.stack([h_new, u_new, v_new]) + vertical_mix * vert

def reference(checkpoints, obs_values, obs_mask, drag):
    rows = jnp.arange(NX).astype(jnp.float32)
    cols = jnp.arange(NY).astype(jnp.float32)
    coriolis = 0.2 + 0.1 * rows / NX
    weight = (1.0 + 2.0 * rows / NX)[:, None] * (1.0 + 2.0 * cols / NY)[None, :]
    adjoint = jnp.zeros((3, NLEV, NX, NY), jnp.float32)
    cost = jnp.zeros((NLEV,), jnp.float32)
    drag_total = jnp.zeros((NLEV,), jnp.float32)
    for seg in reversed(range(NSEG)):
        state = checkpoints[seg].astype(jnp.float32)
        pads = []
        for step in range(SEG):
            padded = jnp.pad(state, ((0, 0), (1, 1), (1, 1), (1, 1)))
            pads.append(padded)
            state = advance(padded, drag, coriolis)
        resid = state[0] - obs_values[seg]
        forcing = weight[None] * obs_mask[seg].astype(jnp.float32) * resid
        cost = cost + 0.5 * lax.optimization_barrier(jnp.sum(forcing * resid, axis=(1, 2)))
        adjoint = adjoint.at[0].add(forcing)
        for step in reversed(range(SEG)):

            def local(padded, rate):
                return advance(padded, rate, coriolis)
            unused, pull = jax.vjp(local, pads[step], drag)
            cot_pad, cot_drag = pull(adjoint)
            drag_total = drag_total + cot_drag
            adjoint = cot_pad[:, 1:-1, 1:-1, 1:-1]
    scale = 1.0 / (NX * NY)
    return (adjoint, cost * scale, drag_total * scale)
```

```python
import functools

import jax
import jax.numpy as jnp
from jax import lax
from jax.experimental import pallas as pl
from jax.experimental.pallas import tpu as pltpu
from jax.sharding import Mesh
from jax.sharding import PartitionSpec as P

LANES = 128
HALO = 10
OHALO = 8
PAD = 8
UNSEEN = 1e9
SEEN_BELOW = 1e8
BF, F32 = jnp.bfloat16, jnp.float32

SEGS = (3, 1, 2, 0)
XT = 7
OT = 9
OBS0 = XT * len(SEGS)
REACH = (OBS0 + 2 * OT, OBS0 + OT, 2 * XT)


def lane_ids(shape):
    return lax.broadcasted_iota(jnp.int32, shape, len(shape) - 1)


def split_bf16(x):
    high = x.astype(BF)
    return high, (x - high.astype(F32)).astype(BF)


def pack(strips, width):
    out = jnp.zeros(strips[0].shape, F32)
    lane = lane_ids(out.shape)
    for j, strip in enumerate(strips):
        start = 2 * width * j
        moved = pltpu.roll(strip, (start + width) % LANES, 1)
        out = jnp.where((lane >= start) & (lane < start + 2 * width), moved, out)
    return out


def unpack(tile, j, width):
    back = pltpu.roll(tile, (-(2 * width * j + width)) % LANES, 1)
    lane = lane_ids(back.shape)
    return jnp.where((lane < width) | (lane >= LANES - width), back, 0.0)


def outgoing(cols, ckpt, obs, mask, drag, send, coded):
    segs, rows, levels = obs.shape[0], obs.shape[1], obs.shape[2]
    lane = lane_ids((levels, LANES))
    low = lane < LANES // 2
    observed = []
    for s in range(segs):
        for r in range(rows):
            value = jnp.where(mask[s, r] > 0, obs[s, r], UNSEEN)
            coded[s * rows + r] = value
            observed.append(value)
    coded[segs * rows] = jnp.broadcast_to(drag[...], (levels, LANES))
    obs_tiles = []
    for pair in (SEGS[:2], SEGS[2:]):
        strips = []
        for s in pair:
            for r in range(rows):
                strips.extend(part.astype(F32) for part in split_bf16(observed[s * rows + r]))
        obs_tiles.append(pack(strips, OHALO).astype(BF))
    zero = jnp.zeros((levels, LANES), F32)
    for c in range(cols):
        strips = []
        for comp in range(3):
            for r in range(rows):
                own = ckpt[comp, r, :, c * LANES : (c + 1) * LANES]
                for z in range(2):
                    send[c, z, comp * rows + r] = own
                left = ckpt[comp, r, :, (c - 1) * LANES : c * LANES].astype(F32) if c else zero
                right = (
                    ckpt[comp, r, :, (c + 1) * LANES : (c + 2) * LANES].astype(F32)
                    if c < cols - 1
                    else zero
                )
                strips.append(jnp.where(low, right, left))
        tiles = [pack(strips, HALO).astype(BF)] + obs_tiles
        for t, tile in enumerate(tiles):
            for z in range(2):
                send[c, z, 6 + t] = tile


def arrange(cols, place, got, coded, theirs, one, two, three):
    col, core = place[1], place[2]
    levels, rows = coded.shape[1], 2
    outs = (one, two, three)

    def put(t, g, tile):
        for out in outs:
            if t < out.shape[0]:
                out[t, g * levels : (g + 1) * levels] = tile

    lane = lane_ids((levels, LANES))
    left = (lane % (2 * OHALO)) < OHALO
    west = jnp.maximum(col - 1, 0)
    east = jnp.minimum(col + 1, cols - 1)
    for g in range(2):
        for k, s in enumerate(SEGS):
            for t in range(XT):
                put(k * XT + t, g, got[s * 2 + g, t])
        mine = core == g
        for k in range(2):
            base = OBS0 + k * OT
            for n, s in enumerate(SEGS[2 * k : 2 * k + 2]):
                for r in range(rows):
                    value = jnp.where(mine, coded[s * rows + r], theirs[s * rows + r])
                    for e, part in enumerate(split_bf16(value)):
                        put(base + (n * rows + r) * 2 + e, g, part)
            strip = jnp.where(
                left, got[west * 2 + g, 7 + k].astype(F32), got[east * 2 + g, 7 + k].astype(F32)
            )
            put(base + OT - 1, g, strip.astype(BF))


def chunk(pair, first, dims, place, coded, theirs, one, r1, r2, r3, swapped, *rest):
    if first:
        lam_out, sums_out, x0, x1, la, lb, obs, decay = rest
    else:
        lam_own, l1, l2, lswap, sums_in, grad, message, x0, x1, la, lb, obs, decay = rest
    total_rows, total_cols = dims
    gx, col, core = place[0], place[1], place[2]
    levels = one.shape[1]
    half = levels // 2
    wide = 2 * LANES
    got = (r1, r2, r3)
    starts = (0, REACH[0], REACH[0] + REACH[1])

    for buf in (x0, x1, la, lb):
        edge = jnp.zeros(buf.shape[:2] + (PAD, wide), F32)
        buf[:, :, :PAD] = edge
        buf[:, :, PAD + levels :] = edge
    for g in range(2):
        k = jnp.where(core == g, coded[coded.shape[0] - 1], theirs[theirs.shape[0] - 1])
        both = jnp.concatenate([k, k], axis=1)
        decay[g * half : (g + 1) * half] = 0.4 - 0.1 * both

    lane = lane_ids((1, wide))
    column = jnp.where(lane < LANES, lane, jnp.where(lane < LANES + HALO, lane, lane - wide))
    held = (lane < LANES + HALO) | (lane >= wide - HALO)
    column = column + col * LANES
    inside = jnp.where(held & (column >= 0) & (column < total_cols), 1.0, 0.0).astype(F32)
    across = inside * (1.0 + 2.0 * column.astype(F32) / total_cols)

    def row_of(i, reach):
        row = gx * 2 + i - reach
        exists = jnp.where((row >= 0) & (row < total_rows), 1.0, 0.0).astype(F32)
        return row.astype(F32), exists

    def tile(b, t, arrays, swap, offsets):
        if b == 0:
            return arrays[0][t].astype(F32)
        mine = arrays[abs(b)][t].astype(F32)
        other = swap[offsets[abs(b) - 1] + t].astype(F32)
        return jnp.where(core == (0 if b < 0 else 1), mine, other)

    def state_tile(b, t):
        return tile(b, t, (one,) + got, swapped, starts)

    def load_state(seg, reach):
        base = SEGS.index(seg) * XT
        blocks = reach // 2
        for b in range(-blocks, blocks + 1):
            strip = state_tile(b, base + 6)
            for comp in range(3):
                for r in range(2):
                    j = comp * 2 + r
                    row = 2 * (b + blocks) + r
                    x0[comp, row, PAD : PAD + levels, :LANES] = state_tile(b, base + j)
                    x0[comp, row, PAD : PAD + levels, LANES:] = unpack(strip, j, HALO)

    def load_obs(seg, reach):
        n = SEGS.index(seg)
        base = OBS0 + (n // 2) * OT
        blocks = reach // 2
        for b in range(-blocks, blocks + 1):
            strip = state_tile(b, base + OT - 1)
            for r in range(2):
                row = 2 * (b + blocks) + r
                j = ((n % 2) * 2 + r) * 2
                obs[row, :, :LANES] = state_tile(b, base + j) + state_tile(b, base + j + 1)
                obs[row, :, LANES:] = unpack(strip, j, OHALO) + unpack(strip, j + 1, OHALO)

    def east(a):
        return pltpu.roll(a, wide - 1, 1)

    def west(a):
        return pltpu.roll(a, 1, 1)

    def here(buf, comp, i, j):
        return buf[comp, i, PAD + 8 * j : PAD + 8 * j + 8]

    def mixed(buf, comp, i, j):
        lo = PAD + 8 * j
        return buf[comp, i, lo + 1 : lo + 9] + buf[comp, i, lo - 1 : lo + 7]

    def step_h(x, i, j):
        h, u, v = here(x, 0, i, j), here(x, 1, i, j), here(x, 2, i, j)
        he, hw, ue, uw = east(h), west(h), east(u), west(u)
        hn, hs = here(x, 0, i + 1, j), here(x, 0, i - 1, j)
        vn, vs = here(x, 2, i + 1, j), here(x, 2, i - 1, j)
        new = (
            0.4 * h
            + 0.05
            * ((hn + hs) + (he + hw) - (ue - uw) - (vn - vs) - (he * ue - hw * uw) - (hn * vn - hs * vs))
            + 0.2 * mixed(x, 0, i, j)
        )
        return new, (h, u, v, he, hw, ue, uw, hn, hs, vn, vs)

    def forward(reach):
        def body(i, carry):
            row, exists = row_of(i, reach - 1)
            mask = inside * exists
            spin = 0.1 * (0.2 + 0.1 * row / total_rows)
            for j in range(levels // 8):
                h_new, (h, u, v, he, hw, ue, uw, hn, hs, vn, vs) = step_h(x0, i + 1, j)
                un, us = here(x0, 1, i + 2, j), here(x0, 1, i, j)
                ve, vw = east(v), west(v)
                keep = decay[8 * j : 8 * j + 8]
                u_new = (
                    keep * u
                    + 0.05 * ((un + us) + (ue + uw) - (he - hw) - u * (ue - uw) - v * (un - us))
                    + spin * v
                    + 0.2 * mixed(x0, 1, i + 1, j)
                )
                v_new = (
                    keep * v
                    + 0.05 * ((vn + vs) + (ve + vw) - (hn - hs) - u * (ve - vw) - v * (vn - vs))
                    - spin * u
                    + 0.2 * mixed(x0, 2, i + 1, j)
                )
                lo = PAD + 8 * j
                x1[0, i, lo : lo + 8] = h_new * mask
                x1[1, i, lo : lo + 8] = u_new * mask
                x1[2, i, lo : lo + 8] = v_new * mask
            return carry

        lax.fori_loop(0, 2 * reach, body, 0)

    def force(reach, add, cost):
        def body(i, carry):
            row, exists = row_of(i, reach)
            scale = across * (exists * (1.0 + 2.0 * row / total_rows))
            own = jnp.where((i >= reach) & (i < reach + 2), 0.5, 0.0).astype(F32)
            new = []
            for j in range(levels // 8):
                h2, _ = step_h(x1, i + 1, j)
                seen = obs[i, 8 * j : 8 * j + 8]
                miss = jnp.where(seen < SEEN_BELOW, h2 - seen, 0.0)
                g = scale * miss
                lo = PAD + 8 * j
                if add:
                    la[0, i, lo : lo + 8] = la[0, i, lo : lo + 8] + g
                else:
                    la[0, i, lo : lo + 8] = g
                    la[1, i, lo : lo + 8] = jnp.zeros_like(g)
                    la[2, i, lo : lo + 8] = jnp.zeros_like(g)
                new.append(carry[j] + own * (g * miss)[:, :LANES])
            return tuple(new)

        return lax.fori_loop(0, 2 * reach + 2, body, cost)

    def backward(lam, x, shift, out, count, reach):
        def body(i, carry):
            row, exists = row_of(i, reach)
            mask = inside * exists
            spin = 0.1 * (0.2 + 0.1 * row / total_rows)
            p = i + shift
            for j in range(levels // 8):
                a, b, c = (here(lam, comp, i + 1, j) for comp in range(3))
                h, u, v = (here(x, comp, p, j) for comp in range(3))
                ae, aw, an, as_ = east(a), west(a), here(lam, 0, i + 2, j), here(lam, 0, i, j)
                be, bw, bn, bs = east(b), west(b), here(lam, 1, i + 2, j), here(lam, 1, i, j)
                ce, cw, cn, cs = east(c), west(c), here(lam, 2, i + 2, j), here(lam, 2, i, j)
                ue, uw, un, us = east(u), west(u), here(x, 1, p + 1, j), here(x, 1, p - 1, j)
                ve, vw, vn, vs = east(v), west(v), here(x, 2, p + 1, j), here(x, 2, p - 1, j)
                keep = decay[8 * j : 8 * j + 8]
                ax, ay = ae - aw, an - as_
                deep = 1.0 + h
                a_new = (
                    0.4 * a
                    + 0.05 * ((an + as_) + (ae + aw) + (be - bw) + (cn - cs) + u * ax + v * ay)
                    + 0.2 * mixed(lam, 0, i + 1, j)
                )
                b_new = (
                    keep * b
                    + 0.05
                    * (
                        (bn + bs)
                        + (be + bw)
                        - b * (ue - uw)
                        + (ue * be - uw * bw)
                        + (vn * bn - vs * bs)
                        - c * (ve - vw)
                        + deep * ax
                    )
                    - spin * c
                    + 0.2 * mixed(lam, 1, i + 1, j)
                )
                c_new = (
                    keep * c
                    + 0.05
                    * (
                        (cn + cs)
                        + (ce + cw)
                        - b * (un - us)
                        + (ue * ce - uw * cw)
                        - c * (vn - vs)
                        + (vn * cn - vs * cs)
                        + deep * ay
                    )
                    + spin * b
                    + 0.2 * mixed(lam, 2, i + 1, j)
                )
                lo = PAD + 8 * j
                out[0, i, lo : lo + 8] = a_new * mask
                out[1, i, lo : lo + 8] = b_new * mask
                out[2, i, lo : lo + 8] = c_new * mask
            return carry

        lax.fori_loop(0, count, body, 0)

    def drag_terms(lam, lrow, x, xrow, total):
        new = []
        for j in range(levels // 8):
            t = total[j]
            for r in range(2):
                for comp in (1, 2):
                    mine = here(lam, comp, lrow + r, j)[:, :LANES]
                    t = t + mine * here(x, comp, xrow + r, j)[:, :LANES]
            new.append(t)
        return new

    zero = tuple(jnp.zeros((8, LANES), F32) for _ in range(levels // 8))
    cost, pulled = zero, list(zero)
    if not first:
        lams = (lam_own, l1, l2)
        for b in range(-2, 3):
            strip = tile(b, 6, lams, lswap, (0, XT))
            for comp in range(3):
                for r in range(2):
                    j = comp * 2 + r
                    row = 2 * (b + 2) + r
                    main = tile(b, j, lams, lswap, (0, XT))
                    la[comp, row, PAD : PAD + levels, :LANES] = main
                    la[comp, row, PAD : PAD + levels, LANES:] = unpack(strip, j, HALO)

    far, near = pair
    load_state(far, 6)
    load_obs(far, 4)
    forward(6)
    cost = force(4, not first, cost)
    pulled = drag_terms(la, 4, x1, 5, pulled)
    backward(la, x1, 2, lb, 8, 3)
    pulled = drag_terms(lb, 3, x0, 6, pulled)
    backward(lb, x0, 4, la, 6, 2)
    load_state(near, 4)
    load_obs(near, 2)
    forward(4)
    cost = force(2, True, cost)
    pulled = drag_terms(la, 2, x1, 3, pulled)
    backward(la, x1, 2, lb, 4, 1)
    pulled = drag_terms(lb, 1, x0, 4, pulled)
    backward(lb, x0, 4, la, 2, 0)

    if first:
        strips = []
        for comp in range(3):
            for r in range(2):
                lam_out[comp * 2 + r] = la[comp, r, PAD : PAD + levels, :LANES]
                strips.append(la[comp, r, PAD : PAD + levels, LANES:])
        lam_out[6] = pack(strips, HALO)
        for j in range(levels // 8):
            sums_out[0, 8 * j : 8 * j + 8] = cost[j]
            sums_out[1, 8 * j : 8 * j + 8] = pulled[j]
    else:
        start = pl.multiple_of(core * half, half)
        for comp in range(3):
            for r in range(2):
                grad[comp, r] = la[comp, r, pl.ds(PAD + start, half), :LANES]
        for j in range(levels // 8):
            obs[0, 8 * j : 8 * j + 8, :LANES] = cost[j] + sums_in[0, 8 * j : 8 * j + 8]
            obs[1, 8 * j : 8 * j + 8, :LANES] = pulled[j] + sums_in[1, 8 * j : 8 * j + 8]
        area = 1.0 / (total_rows * total_cols)
        line = jnp.zeros((1, LANES), F32)
        for k, factor in ((0, area), (1, -0.1 * area)):
            part = jnp.sum(obs[k, pl.ds(start, half), :LANES], axis=1, keepdims=True) * factor
            level = lax.broadcasted_iota(jnp.int32, (half, LANES), 0) + k * half
            line = line + jnp.sum(
                jnp.where(level == lane_ids((half, LANES)), part, 0.0), axis=0, keepdims=True
            )
        for n in range(message.shape[0]):
            message[n] = jnp.broadcast_to(line, message.shape[1:])


def vmem():
    return pl.BlockSpec(memory_space=pltpu.VMEM)


def smem():
    return pl.BlockSpec(memory_space=pltpu.SMEM)


def call(kernel, outs, places, vmems, scratch=(), limit=None):
    return pl.pallas_call(
        kernel,
        out_shape=outs,
        in_specs=[smem()] * len(places) + [vmem()] * len(vmems),
        out_specs=jax.tree.map(lambda _: vmem(), outs),
        scratch_shapes=list(scratch),
        compiler_params=pltpu.CompilerParams(vmem_limit_bytes=limit),
    )(*places, *vmems)


def on_device(checkpoints, obs_values, obs_mask, drag):
    segs, levels, rows, lanes = obs_values.shape
    cols, cores = lax.axis_size("col"), lax.axis_size("gz")
    outer, inner = lax.axis_size("gxo"), lax.axis_size("gxi")
    lat = outer * inner
    dims = (rows * lat, lanes * cols)
    place = jnp.stack(
        [lax.axis_index("gxo") * inner + lax.axis_index("gxi"), lax.axis_index("col"), lax.axis_index("gz")]
    ).astype(jnp.int32)

    def sds(shape, dtype=F32):
        return jax.ShapeDtypeStruct(shape, dtype)

    def toward(block, distance):
        route = []
        for i in range(lat):
            for core, step in ((0, distance), (1, -distance)):
                if 0 <= i + step < lat:
                    route.append((i * cores + core, (i + step) * cores + core))
        return lax.ppermute(block, ("gxo", "gxi", "gz"), route)

    def swap(block):
        return lax.ppermute(block, "gz", [(0, 1), (1, 0)])

    send, coded = call(
        functools.partial(outgoing, cols),
        (sds((cols, cores, 9, levels, LANES), BF), sds((segs * rows + 1, levels, LANES))),
        (),
        (
            checkpoints[0].transpose(0, 2, 1, 3),
            obs_values.transpose(0, 2, 1, 3),
            obs_mask.transpose(0, 2, 1, 3),
            drag[:, None],
        ),
    )
    theirs = swap(coded)
    got = lax.all_to_all(
        send.reshape(cols * cores, 9, levels, LANES), ("col", "gz"), 0, 0, tiled=True
    )
    full = levels * cores
    ones = call(
        functools.partial(arrange, cols),
        tuple(sds((n, full, LANES), BF) for n in REACH),
        (place,),
        (got, coded, theirs),
    )
    came = [toward(block, d + 1) for d, block in enumerate(ones)]
    swapped = swap(jnp.concatenate(came))

    def scratch():
        return [
            pltpu.VMEM((3, 14, full + 2 * PAD, 2 * LANES), F32),
            pltpu.VMEM((3, 12, full + 2 * PAD, 2 * LANES), F32),
            pltpu.VMEM((3, 10, full + 2 * PAD, 2 * LANES), F32),
            pltpu.VMEM((3, 8, full + 2 * PAD, 2 * LANES), F32),
            pltpu.VMEM((10, full, 2 * LANES), F32),
            pltpu.VMEM((full, 2 * LANES), F32),
        ]

    data = (coded, theirs, ones[0], *came, swapped)
    lam, sums = call(
        functools.partial(chunk, (3, 2), True, dims),
        (sds((XT, full, LANES)), sds((2, full, LANES))),
        (place,),
        data,
        scratch(),
    )
    near, next_ = toward(lam, 1), toward(lam, 2)
    lswap = swap(jnp.concatenate([near, next_]))
    team = inner * cols
    grad, message = call(
        functools.partial(chunk, (1, 0), False, dims),
        (sds((3, rows, levels, LANES)), sds((team, 8, LANES))),
        (place,),
        data + (lam, near, next_, lswap, sums),
        scratch(),
    )
    near_sum = jnp.sum(lax.all_to_all(message, ("gxi", "col"), 0, 0, tiled=True), axis=0)
    spread = jnp.broadcast_to(near_sum, (outer,) + near_sum.shape)
    total = jnp.sum(lax.all_to_all(spread, "gxo", 0, 0, tiled=True), axis=0)[0]
    return grad.transpose(0, 2, 1, 3), total[:levels], total[levels : 2 * levels]


def solution(mesh):
    inner = 4
    sizes = dict(mesh.shape)
    fine = Mesh(
        mesh.devices.reshape(sizes["ens"], sizes["gx"] // inner, inner, sizes["col"], sizes["gz"]),
        ("ens", "gxo", "gxi", "col", "gz"),
    )
    lat = ("gxo", "gxi")
    return jax.shard_map(
        on_device,
        mesh=fine,
        in_specs=(
            P(("ens", "col"), None, "gz", lat, None),
            P("ens", "gz", lat, "col"),
            P("ens", "gz", lat, "col"),
            P(("ens", "gz")),
        ),
        out_specs=(P("ens", "gz", lat, "col"), P(("ens", "gz")), P(("ens", "gz"))),
        check_vma=False,
    )
```

```python
import functools

import jax
import jax.numpy as jnp
from jax import lax
from jax.experimental import pallas as pl
from jax.experimental.pallas import tpu as pltpu
from jax.sharding import Mesh
from jax.sharding import PartitionSpec as P

LANES = 128
HALO = 10
OHALO = 8
PAD = 8
UNSEEN = 1e9
SEEN_BELOW = 1e8
BF, F32 = jnp.bfloat16, jnp.float32

SEGS = (3, 1, 2, 0)
XT = 7
OT = 9
OBS0 = XT * len(SEGS)
REACH = (OBS0 + 2 * OT, OBS0 + OT, 2 * XT)


def lane_ids(shape):
    return lax.broadcasted_iota(jnp.int32, shape, len(shape) - 1)


def split_bf16(x):
    high = x.astype(BF)
    return high, (x - high.astype(F32)).astype(BF)


def pack(strips, width):
    out = jnp.zeros(strips[0].shape, F32)
    lane = lane_ids(out.shape)
    for j, strip in enumerate(strips):
        start = 2 * width * j
        moved = pltpu.roll(strip, (start + width) % LANES, 1)
        out = jnp.where((lane >= start) & (lane < start + 2 * width), moved, out)
    return out


def unpack(tile, j, width):
    back = pltpu.roll(tile, (-(2 * width * j + width)) % LANES, 1)
    lane = lane_ids(back.shape)
    return jnp.where((lane < width) | (lane >= LANES - width), back, 0.0)


def outgoing(cols, drag, ckpt, obs, mask, send, coded, wide):
    segs, rows = obs.shape[0], 2
    levels = obs.shape[1] // rows
    lane = lane_ids((levels, LANES))
    low = lane < LANES // 2
    for comp in range(3):
        wide[comp] = ckpt[comp].astype(F32)

    def plane(comp, r, c):
        return wide[comp, pl.ds(c * rows + r, levels, stride=rows * cols), :]

    observed = []
    for s in range(segs):
        for r in range(rows):
            spot = pl.ds(r, levels, stride=rows)
            value = jnp.where(mask[s, spot, :] > 0, obs[s, spot, :], UNSEEN)
            coded[s * rows + r] = value
            observed.append(value)
    level = lax.broadcasted_iota(jnp.int32, (levels, LANES), 0)
    rates = jnp.zeros((levels, LANES), F32)
    for k in range(levels):
        rates = jnp.where(level == k, drag[k], rates)
    coded[segs * rows] = rates
    obs_tiles = []
    for pair in (SEGS[:2], SEGS[2:]):
        strips = []
        for s in pair:
            for r in range(rows):
                strips.extend(part.astype(F32) for part in split_bf16(observed[s * rows + r]))
        obs_tiles.append(pack(strips, OHALO).astype(BF))
    zero = jnp.zeros((levels, LANES), F32)
    for c in range(cols):
        strips = []
        for comp in range(3):
            for r in range(rows):
                own = plane(comp, r, c).astype(BF)
                for z in range(2):
                    send[c, z, comp * rows + r] = own
                left = plane(comp, r, c - 1) if c else zero
                right = plane(comp, r, c + 1) if c < cols - 1 else zero
                strips.append(jnp.where(low, right, left))
        tiles = [pack(strips, HALO).astype(BF)] + obs_tiles
        for t, tile in enumerate(tiles):
            for z in range(2):
                send[c, z, 6 + t] = tile


def arrange(cols, place, got, coded, theirs, one, two, three):
    col, core = place[1], place[2]
    levels, rows = coded.shape[1], 2
    outs = (one, two, three)

    def put(t, g, tile):
        for out in outs:
            if t < out.shape[0]:
                out[t, g * levels : (g + 1) * levels] = tile

    lane = lane_ids((levels, LANES))
    left = (lane % (2 * OHALO)) < OHALO
    west = jnp.maximum(col - 1, 0)
    east = jnp.minimum(col + 1, cols - 1)
    for g in range(2):
        for k, s in enumerate(SEGS):
            for t in range(XT):
                put(k * XT + t, g, got[s * 2 + g, t])
        mine = core == g
        for k in range(2):
            base = OBS0 + k * OT
            for n, s in enumerate(SEGS[2 * k : 2 * k + 2]):
                for r in range(rows):
                    value = jnp.where(mine, coded[s * rows + r], theirs[s * rows + r])
                    for e, part in enumerate(split_bf16(value)):
                        put(base + (n * rows + r) * 2 + e, g, part)
            strip = jnp.where(
                left, got[west * 2 + g, 7 + k].astype(F32), got[east * 2 + g, 7 + k].astype(F32)
            )
            put(base + OT - 1, g, strip.astype(BF))


def chunk(pair, first, dims, place, coded, theirs, one, r1, r2, r3, swapped, *rest):
    if first:
        lam_out, sums_out, x0, x1, la, lb, obs, decay = rest
    else:
        lam_own, l1, l2, lswap, sums_in, grad, message, x0, x1, la, lb, obs, decay = rest
    total_rows, total_cols = dims
    gx, col, core = place[0], place[1], place[2]
    levels = one.shape[1]
    half = levels // 2
    wide = 2 * LANES
    got = (r1, r2, r3)
    starts = (0, REACH[0], REACH[0] + REACH[1])

    for buf in (x0, x1, la, lb):
        edge = jnp.zeros(buf.shape[:2] + (PAD, wide), F32)
        buf[:, :, :PAD] = edge
        buf[:, :, PAD + levels :] = edge
    for g in range(2):
        k = jnp.where(core == g, coded[coded.shape[0] - 1], theirs[theirs.shape[0] - 1])
        both = jnp.concatenate([k, k], axis=1)
        decay[g * half : (g + 1) * half] = 0.4 - 0.1 * both

    lane = lane_ids((1, wide))
    column = jnp.where(lane < LANES, lane, jnp.where(lane < LANES + HALO, lane, lane - wide))
    held = (lane < LANES + HALO) | (lane >= wide - HALO)
    column = column + col * LANES
    inside = jnp.where(held & (column >= 0) & (column < total_cols), 1.0, 0.0).astype(F32)
    across = inside * (1.0 + 2.0 * column.astype(F32) / total_cols)

    def row_of(i, reach):
        row = gx * 2 + i - reach
        exists = jnp.where((row >= 0) & (row < total_rows), 1.0, 0.0).astype(F32)
        return row.astype(F32), exists

    def tile(b, t, arrays, swap, offsets):
        if b == 0:
            return arrays[0][t].astype(F32)
        mine = arrays[abs(b)][t].astype(F32)
        other = swap[offsets[abs(b) - 1] + t].astype(F32)
        return jnp.where(core == (0 if b < 0 else 1), mine, other)

    def state_tile(b, t):
        return tile(b, t, (one,) + got, swapped, starts)

    def load_state(seg, reach):
        base = SEGS.index(seg) * XT
        blocks = reach // 2
        for b in range(-blocks, blocks + 1):
            strip = state_tile(b, base + 6)
            for comp in range(3):
                for r in range(2):
                    j = comp * 2 + r
                    row = 2 * (b + blocks) + r
                    x0[comp, row, PAD : PAD + levels, :LANES] = state_tile(b, base + j)
                    x0[comp, row, PAD : PAD + levels, LANES:] = unpack(strip, j, HALO)

    def load_obs(seg, reach):
        n = SEGS.index(seg)
        base = OBS0 + (n // 2) * OT
        blocks = reach // 2
        for b in range(-blocks, blocks + 1):
            strip = state_tile(b, base + OT - 1)
            for r in range(2):
                row = 2 * (b + blocks) + r
                j = ((n % 2) * 2 + r) * 2
                obs[row, :, :LANES] = state_tile(b, base + j) + state_tile(b, base + j + 1)
                obs[row, :, LANES:] = unpack(strip, j, OHALO) + unpack(strip, j + 1, OHALO)

    def east(a):
        return pltpu.roll(a, wide - 1, 1)

    def west(a):
        return pltpu.roll(a, 1, 1)

    def here(buf, comp, i, j):
        return buf[comp, i, PAD + 8 * j : PAD + 8 * j + 8]

    def mixed(buf, comp, i, j):
        lo = PAD + 8 * j
        return buf[comp, i, lo + 1 : lo + 9] + buf[comp, i, lo - 1 : lo + 7]

    def step_h(x, i, j):
        h, u, v = here(x, 0, i, j), here(x, 1, i, j), here(x, 2, i, j)
        he, hw, ue, uw = east(h), west(h), east(u), west(u)
        hn, hs = here(x, 0, i + 1, j), here(x, 0, i - 1, j)
        vn, vs = here(x, 2, i + 1, j), here(x, 2, i - 1, j)
        new = (
            0.4 * h
            + 0.05
            * ((hn + hs) + (he + hw) - (ue - uw) - (vn - vs) - (he * ue - hw * uw) - (hn * vn - hs * vs))
            + 0.2 * mixed(x, 0, i, j)
        )
        return new, (h, u, v, he, hw, ue, uw, hn, hs, vn, vs)

    def forward(reach):
        def body(i, carry):
            row, exists = row_of(i, reach - 1)
            mask = inside * exists
            spin = 0.1 * (0.2 + 0.1 * row / total_rows)
            for j in range(levels // 8):
                h_new, (h, u, v, he, hw, ue, uw, hn, hs, vn, vs) = step_h(x0, i + 1, j)
                un, us = here(x0, 1, i + 2, j), here(x0, 1, i, j)
                ve, vw = east(v), west(v)
                keep = decay[8 * j : 8 * j + 8]
                u_new = (
                    keep * u
                    + 0.05 * ((un + us) + (ue + uw) - (he - hw) - u * (ue - uw) - v * (un - us))
                    + spin * v
                    + 0.2 * mixed(x0, 1, i + 1, j)
                )
                v_new = (
                    keep * v
                    + 0.05 * ((vn + vs) + (ve + vw) - (hn - hs) - u * (ve - vw) - v * (vn - vs))
                    - spin * u
                    + 0.2 * mixed(x0, 2, i + 1, j)
                )
                lo = PAD + 8 * j
                x1[0, i, lo : lo + 8] = h_new * mask
                x1[1, i, lo : lo + 8] = u_new * mask
                x1[2, i, lo : lo + 8] = v_new * mask
            return carry

        lax.fori_loop(0, 2 * reach, body, 0)

    def force(reach, add, cost):
        def body(i, carry):
            row, exists = row_of(i, reach)
            scale = across * (exists * (1.0 + 2.0 * row / total_rows))
            own = jnp.where((i >= reach) & (i < reach + 2), 0.5, 0.0).astype(F32)
            new = []
            for j in range(levels // 8):
                h2, _ = step_h(x1, i + 1, j)
                seen = obs[i, 8 * j : 8 * j + 8]
                miss = jnp.where(seen < SEEN_BELOW, h2 - seen, 0.0)
                g = scale * miss
                lo = PAD + 8 * j
                if add:
                    la[0, i, lo : lo + 8] = la[0, i, lo : lo + 8] + g
                else:
                    la[0, i, lo : lo + 8] = g
                    la[1, i, lo : lo + 8] = jnp.zeros_like(g)
                    la[2, i, lo : lo + 8] = jnp.zeros_like(g)
                new.append(carry[j] + own * (g * miss)[:, :LANES])
            return tuple(new)

        return lax.fori_loop(0, 2 * reach + 2, body, cost)

    def backward(lam, x, shift, out, count, reach):
        def body(i, carry):
            row, exists = row_of(i, reach)
            mask = inside * exists
            spin = 0.1 * (0.2 + 0.1 * row / total_rows)
            p = i + shift
            for j in range(levels // 8):
                a, b, c = (here(lam, comp, i + 1, j) for comp in range(3))
                h, u, v = (here(x, comp, p, j) for comp in range(3))
                ae, aw, an, as_ = east(a), west(a), here(lam, 0, i + 2, j), here(lam, 0, i, j)
                be, bw, bn, bs = east(b), west(b), here(lam, 1, i + 2, j), here(lam, 1, i, j)
                ce, cw, cn, cs = east(c), west(c), here(lam, 2, i + 2, j), here(lam, 2, i, j)
                ue, uw, un, us = east(u), west(u), here(x, 1, p + 1, j), here(x, 1, p - 1, j)
                ve, vw, vn, vs = east(v), west(v), here(x, 2, p + 1, j), here(x, 2, p - 1, j)
                keep = decay[8 * j : 8 * j + 8]
                ax, ay = ae - aw, an - as_
                deep = 1.0 + h
                a_new = (
                    0.4 * a
                    + 0.05 * ((an + as_) + (ae + aw) + (be - bw) + (cn - cs) + u * ax + v * ay)
                    + 0.2 * mixed(lam, 0, i + 1, j)
                )
                b_new = (
                    keep * b
                    + 0.05
                    * (
                        (bn + bs)
                        + (be + bw)
                        - b * (ue - uw)
                        + (ue * be - uw * bw)
                        + (vn * bn - vs * bs)
                        - c * (ve - vw)
                        + deep * ax
                    )
                    - spin * c
                    + 0.2 * mixed(lam, 1, i + 1, j)
                )
                c_new = (
                    keep * c
                    + 0.05
                    * (
                        (cn + cs)
                        + (ce + cw)
                        - b * (un - us)
                        + (ue * ce - uw * cw)
                        - c * (vn - vs)
                        + (vn * cn - vs * cs)
                        + deep * ay
                    )
                    + spin * b
                    + 0.2 * mixed(lam, 2, i + 1, j)
                )
                lo = PAD + 8 * j
                out[0, i, lo : lo + 8] = a_new * mask
                out[1, i, lo : lo + 8] = b_new * mask
                out[2, i, lo : lo + 8] = c_new * mask
            return carry

        lax.fori_loop(0, count, body, 0)

    def drag_terms(lam, lrow, x, xrow, total):
        new = []
        for j in range(levels // 8):
            t = total[j]
            for r in range(2):
                for comp in (1, 2):
                    mine = here(lam, comp, lrow + r, j)[:, :LANES]
                    t = t + mine * here(x, comp, xrow + r, j)[:, :LANES]
            new.append(t)
        return new

    zero = tuple(jnp.zeros((8, LANES), F32) for _ in range(levels // 8))
    cost, pulled = zero, list(zero)
    if not first:
        lams = (lam_own, l1, l2)
        for b in range(-2, 3):
            strip = tile(b, 6, lams, lswap, (0, XT))
            for comp in range(3):
                for r in range(2):
                    j = comp * 2 + r
                    row = 2 * (b + 2) + r
                    main = tile(b, j, lams, lswap, (0, XT))
                    la[comp, row, PAD : PAD + levels, :LANES] = main
                    la[comp, row, PAD : PAD + levels, LANES:] = unpack(strip, j, HALO)

    far, near = pair
    load_state(far, 6)
    load_obs(far, 4)
    forward(6)
    cost = force(4, not first, cost)
    pulled = drag_terms(la, 4, x1, 5, pulled)
    backward(la, x1, 2, lb, 8, 3)
    pulled = drag_terms(lb, 3, x0, 6, pulled)
    backward(lb, x0, 4, la, 6, 2)
    load_state(near, 4)
    load_obs(near, 2)
    forward(4)
    cost = force(2, True, cost)
    pulled = drag_terms(la, 2, x1, 3, pulled)
    backward(la, x1, 2, lb, 4, 1)
    pulled = drag_terms(lb, 1, x0, 4, pulled)
    backward(lb, x0, 4, la, 2, 0)

    if first:
        strips = []
        for comp in range(3):
            for r in range(2):
                lam_out[comp * 2 + r] = la[comp, r, PAD : PAD + levels, :LANES]
                strips.append(la[comp, r, PAD : PAD + levels, LANES:])
        lam_out[6] = pack(strips, HALO)
        for j in range(levels // 8):
            sums_out[0, 8 * j : 8 * j + 8] = cost[j]
            sums_out[1, 8 * j : 8 * j + 8] = pulled[j]
    else:
        start = pl.multiple_of(core * half, half)
        for comp in range(3):
            for r in range(2):
                grad[comp, r] = la[comp, r, pl.ds(PAD + start, half), :LANES]
        for j in range(levels // 8):
            obs[0, 8 * j : 8 * j + 8, :LANES] = cost[j] + sums_in[0, 8 * j : 8 * j + 8]
            obs[1, 8 * j : 8 * j + 8, :LANES] = pulled[j] + sums_in[1, 8 * j : 8 * j + 8]
        area = 1.0 / (total_rows * total_cols)
        line = jnp.zeros((1, LANES), F32)
        for k, factor in ((0, area), (1, -0.1 * area)):
            part = jnp.sum(obs[k, pl.ds(start, half), :LANES], axis=1, keepdims=True) * factor
            level = lax.broadcasted_iota(jnp.int32, (half, LANES), 0) + k * half
            line = line + jnp.sum(
                jnp.where(level == lane_ids((half, LANES)), part, 0.0), axis=0, keepdims=True
            )
        for n in range(message.shape[0]):
            message[n] = jnp.broadcast_to(line, message.shape[1:])


def vmem():
    return pl.BlockSpec(memory_space=pltpu.VMEM)


def smem():
    return pl.BlockSpec(memory_space=pltpu.SMEM)


def call(kernel, outs, places, vmems, scratch=(), limit=None):
    return pl.pallas_call(
        kernel,
        out_shape=outs,
        in_specs=[smem()] * len(places) + [vmem()] * len(vmems),
        out_specs=jax.tree.map(lambda _: vmem(), outs),
        scratch_shapes=list(scratch),
        compiler_params=pltpu.CompilerParams(vmem_limit_bytes=limit),
    )(*places, *vmems)


def on_device(checkpoints, obs_values, obs_mask, drag):
    segs, levels, rows, lanes = obs_values.shape
    cols, cores = lax.axis_size("col"), lax.axis_size("gz")
    outer, inner = lax.axis_size("gxo"), lax.axis_size("gxi")
    lat = outer * inner
    dims = (rows * lat, lanes * cols)
    place = jnp.stack(
        [lax.axis_index("gxo") * inner + lax.axis_index("gxi"), lax.axis_index("col"), lax.axis_index("gz")]
    ).astype(jnp.int32)

    def sds(shape, dtype=F32):
        return jax.ShapeDtypeStruct(shape, dtype)

    def toward(block, distance):
        route = []
        for i in range(lat):
            for core, step in ((0, distance), (1, -distance)):
                if 0 <= i + step < lat:
                    route.append((i * cores + core, (i + step) * cores + core))
        return lax.ppermute(block, ("gxo", "gxi", "gz"), route)

    def swap(block):
        return lax.ppermute(block, "gz", [(0, 1), (1, 0)])

    send, coded = call(
        functools.partial(outgoing, cols),
        (sds((cols, cores, 9, levels, LANES), BF), sds((segs * rows + 1, levels, LANES))),
        (drag,),
        (
            checkpoints.reshape(3, levels, rows, cols, lanes)
            .transpose(0, 1, 3, 2, 4)
            .reshape(3, levels * cols * rows, lanes),
            obs_values.reshape(segs, levels * rows, lanes),
            obs_mask.reshape(segs, levels * rows, lanes),
        ),
        [pltpu.VMEM((3, levels * cols * rows, LANES), F32)],
    )
    theirs = swap(coded)
    got = lax.all_to_all(
        send.reshape(cols * cores, 9, levels, LANES), ("col", "gz"), 0, 0, tiled=True
    )
    full = levels * cores
    ones = call(
        functools.partial(arrange, cols),
        tuple(sds((n, full, LANES), BF) for n in REACH),
        (place,),
        (got, coded, theirs),
        (),
        4 << 20,
    )
    came = [toward(block, 3 - d) for d, block in enumerate(ones[::-1])][::-1]
    swapped = swap(jnp.concatenate(came))

    def scratch():
        return [
            pltpu.VMEM((3, 14, full + 2 * PAD, 2 * LANES), F32),
            pltpu.VMEM((3, 12, full + 2 * PAD, 2 * LANES), F32),
            pltpu.VMEM((3, 10, full + 2 * PAD, 2 * LANES), F32),
            pltpu.VMEM((3, 8, full + 2 * PAD, 2 * LANES), F32),
            pltpu.VMEM((10, full, 2 * LANES), F32),
            pltpu.VMEM((full, 2 * LANES), F32),
        ]

    data = (coded, theirs, ones[0], *came, swapped)
    lam, sums = call(
        functools.partial(chunk, (3, 2), True, dims),
        (sds((XT, full, LANES)), sds((2, full, LANES))),
        (place,),
        data,
        scratch(),
        14 << 20,
    )
    near, next_ = toward(lam, 1), toward(lam, 2)
    lswap = swap(jnp.concatenate([near, next_]))
    team = inner * cols
    grad, message = call(
        functools.partial(chunk, (1, 0), False, dims),
        (sds((3, rows, levels, LANES)), sds((team, 8, LANES))),
        (place,),
        data + (lam, near, next_, lswap, sums),
        scratch(),
        14 << 20,
    )
    near_sum = jnp.sum(lax.all_to_all(message, ("gxi", "col"), 0, 0, tiled=True), axis=0)
    total = lax.psum(near_sum, "gxo")[0]
    return grad.transpose(0, 2, 1, 3), total[:levels], total[levels : 2 * levels]


def solution(mesh):
    inner = 4
    sizes = dict(mesh.shape)
    fine = Mesh(
        mesh.devices.reshape(sizes["ens"], sizes["gx"] // inner, inner, sizes["col"], sizes["gz"]),
        ("ens", "gxo", "gxi", "col", "gz"),
    )
    lat = ("gxo", "gxi")
    return jax.shard_map(
        on_device,
        mesh=fine,
        in_specs=(
            P(("ens", "col"), None, "gz", lat, None),
            P("ens", "gz", lat, "col"),
            P("ens", "gz", lat, "col"),
            P(("ens", "gz")),
        ),
        out_specs=(P("ens", "gz", lat, "col"), P(("ens", "gz")), P(("ens", "gz"))),
        check_vma=False,
    )
```
